256 devices in a mesh: shard: 32 (over z, x), width: 2 (over core), unit: 4 (over y).
Axes of the slice: x: 4, y: 4, z: 8, core: 2. Of those that a mesh axis runs over, the one named last changes fastest.
Arguments:
- w_gate: bfloat16 [14336, 14336], P(('unit', 'shard'), 'width'), parts along dimension 0, may hold values from -0.1875 to 0.1875
- low_gate: bfloat16 [14336, 64], P(('unit', 'shard')), parts along dimension 0, may hold values from -0.09375 to 0.09375
- high_gate: bfloat16 [256, 14336], P('unit', 'width'), parts along dimension 0, may hold values from -0.75 to 0.75
- w_up: bfloat16 [14336, 14336], P(('unit', 'shard'), 'width'), parts along dimension 0, may hold values from -0.1875 to 0.1875
- low_up: bfloat16 [14336, 64], P(('unit', 'shard')), parts along dimension 0, may hold values from -0.09375 to 0.09375
- high_up: bfloat16 [256, 14336], P('unit', 'width'), parts along dimension 0, may hold values from -0.75 to 0.75
- norm_train: float32 [14336], P(('unit', 'shard', 'width')), parts along dimension 0, may hold values from 0.25 to 1.75
- norm_step: float32 [14336], P(('unit', 'shard', 'width')), parts along dimension 0, may hold values from -0.3 to 0.3
Outputs:
- serve_gate: bfloat16 [14336, 14336], P('unit', ('width', 'shard')), parts along dimension 0
- serve_up: bfloat16 [14336, 14336], P('unit', ('width', 'shard')), parts along dimension 0
- column_gate: float32 [57344], P(('unit', 'width', 'shard')), parts along dimension 0
- column_up: float32 [57344], P(('unit', 'width', 'shard')), parts along dimension 0
- serve_norm: bfloat16 [14336], P('unit'), parts along dimension 0
The draws below stay inside these ranges and needn't reach their ends.
There are 4 independent parts, one for each index of `unit`. The reference program is written for one: setup_inputs(seed, part) draws one part's arguments, and reference() takes and returns one part's arrays. A program takes and returns all parts, laid end to end along the dimension named above; each array names one. Nothing has to cross between parts.
All inputs are finite; a program needn't handle non-finite values. Where the reference program divides by a largest or mean magnitude, that divisor is 1e-20 or more.
Results may differ from the reference program's by a relative error of at most 0.001.
Values may be sent and summed in bfloat16 or wider, within the bound.
A program may use at most 64 MiB of HBM per device.

```python
import jax
import jax.numpy as jnp

D_MODEL = 3584
D_INNER = 14336
RANK = 64


def spiked(array, stream_key, source, target, blocks, factor):
    def block_of(dim):
        return (jnp.arange(array.shape[dim]) // (array.shape[dim] // blocks)).reshape((-1,) + (1,) * (array.ndim - 1 - dim))

    first = jax.random.permutation(stream_key, blocks)[block_of(target)]
    other_side = (block_of(target) + blocks // 2) % blocks
    return jnp.where((block_of(source) == first) | (block_of(source) == other_side), factor * array, array)


def levels(key, shape, split, low, largest):
    level, own = 1.0, jax.random.fold_in(key, 6)
    for axis_at, blocks in split:
        draws = jnp.exp(jax.random.uniform(jax.random.fold_in(own, axis_at), (blocks,), jnp.float32, low / len(split), largest / len(split)))
        level = level * jnp.repeat(draws, shape[axis_at] // blocks).reshape([-1 if axis == axis_at else 1 for axis in range(len(shape))])
    return level


def bell_draw(rng, dims, width, limit, pieces=(), kind=jnp.bfloat16):
    entries = width * jax.random.normal(rng, dims, jnp.float32)
    if pieces:
        entries = entries * levels(rng, dims, pieces, -0.22, 0.18)
    return jnp.clip(entries, -limit, limit).astype(kind)


def noise_with(own_key, extent, scale, bound, split, heavy, held_as=jnp.bfloat16):
    values = scale * jax.random.normal(own_key, extent, jnp.float32)
    if split:
        values = values * levels(own_key, extent, split, -0.22, 0.18)
    return jnp.clip(spiked(values, jax.random.fold_in(own_key, 3), *heavy), -bound, bound).astype(held_as)


def setup_inputs(seed: int = 0, part: int = 0) -> dict:
    keys = jax.random.split(jax.random.key(seed), 9)
    own_keys = jax.random.split(jax.random.fold_in(keys[8], part), 9)
    return {
        "w_gate": noise_with(own_keys[0], (D_MODEL, D_INNER), D_MODEL ** -0.5, 0.1875, ((0, 32), (1, 2)), (0, 1, 32, 2.75)),
        "low_gate": bell_draw(own_keys[1], (D_MODEL, RANK), D_MODEL ** -0.5, 0.09375, ((0, 32),)),
        "high_gate": bell_draw(own_keys[2], (RANK, D_INNER), RANK ** -0.5, 0.75, ((1, 2),)),
        "w_up": noise_with(own_keys[3], (D_MODEL, D_INNER), D_MODEL ** -0.5, 0.1875, ((0, 32), (1, 2)), (0, 1, 32, 2.75)),
        "low_up": bell_draw(own_keys[4], (D_MODEL, RANK), D_MODEL ** -0.5, 0.09375, ((0, 32),)),
        "high_up": bell_draw(own_keys[5], (RANK, D_INNER), RANK ** -0.5, 0.75, ((1, 2),)),
        "norm_train": jnp.clip(1.0 + 0.15 * jax.random.normal(own_keys[6], (D_MODEL,), jnp.float32), 0.25, 1.75),
        "norm_step": jnp.clip(jax.random.uniform(own_keys[7], (D_MODEL,), jnp.float32, -0.3, 0.3) * levels(own_keys[7], (D_MODEL,), ((0, 64),), -0.4, 0.0), -0.3, 0.3),
    }


mix_rate = 0.5


def reference(w_gate, low_gate, high_gate, w_up, low_up, high_up, norm_train, norm_step):
    fresh_gate = w_gate.astype(jnp.float32) + mix_rate * jnp.dot(low_gate, high_gate, preferred_element_type=jnp.float32)
    fresh_up = w_up.astype(jnp.float32) + mix_rate * jnp.dot(low_up, high_up, preferred_element_type=jnp.float32)
    column_gate = jnp.max(jnp.abs(fresh_gate), axis=0)
    serve_gate = (fresh_gate / column_gate).astype(jnp.bfloat16)
    column_up = jnp.max(jnp.abs(fresh_up), axis=0)
    serve_up = (fresh_up / column_up).astype(jnp.bfloat16)
    serve_norm = (norm_train + norm_step).astype(jnp.bfloat16)
    return serve_gate, serve_up, column_gate, column_up, serve_norm
```

```python
import jax
import jax.numpy as jnp
from jax import lax
from jax.experimental import pallas as pl
from jax.experimental.pallas import tpu as pltpu
from jax.sharding import PartitionSpec as P

MESH = pl.DeviceIdType.MESH
NZ, NX = 8, 4
ROWS = 112
COLS = 224
RANK = 64
PLANE = NX * COLS
LANES = 128
NEAR = 2 * LANES
WIDE = 3 * LANES
TOTAL = NZ * NX * ROWS
NORM = 56
SLOT = 4 * LANES
HALF = SLOT - NX * ROWS
mix_rate = 0.5


def tile_of(x):
    return (7 * x) // 4


ORDER = (1, 7, 2, 6, 3, 5, 4)
EARLY = ((1, 1), (7, 1))
PIECES = [
    (dz, a, 0, ROWS)
    for dz, a in (
        (1, 0), (7, 0), (4, 0), (2, 0), (6, 0), (3, 0), (5, 0), (4, 1), (3, 1), (5, 1), (2, 1), (6, 1),
    )
]
OWN = [(0, a, 0, ROWS) for a in range(2)]
ALL = OWN + PIECES


def exchange_kernel(
    w_gate,
    low_gate,
    high_gate,
    w_up,
    low_up,
    high_up,
    norm_train,
    norm_step,
    fresh_gate,
    fresh_up,
    peak,
    norm_out,
    zbuf,
    pack,
    xbuf,
    early,
    earlypack,
    earlyrow,
    lowown,
    lowbuf,
    lowrows,
    normbuf,
    hbuf,
    hturn,
    pick,
    hcols,
    norm_abs,
    norm_acc,
    local_sem,
    zs,
    zr,
    xs,
    xr,
    lzs,
    lzr,
    lxs,
    lxr,
    nzs,
    nzr,
    nxs,
    nxr,
    ds,
    dr,
    exs,
    exr,
    ezs,
    ezr,
):
    place = lax.axis_index("shard")
    core = lax.axis_index("width")
    z, x = place // NX, lax.rem(place, NX)
    weights = (w_gate, w_up)
    fresh = (fresh_gate, fresh_up)

    def at(dz, dx):
        return lax.rem(z + dz, NZ) * NX + lax.rem(x + dx, NX)

    def zpeer(dz):
        return {"shard": at(dz, 0)}

    def xpeer(dx):
        return {"shard": at(0, dx)}

    partner = {"width": 1 - core}

    def remote(source, target, send, receive, peer):
        return pltpu.make_async_remote_copy(
            src_ref=source,
            dst_ref=target,
            send_sem=send,
            recv_sem=receive,
            device_id=peer,
            device_id_type=MESH,
        )

    barrier = pltpu.get_barrier_semaphore()
    for dz in range(1, NZ):
        pl.semaphore_signal(barrier, inc=1, device_id=zpeer(dz), device_id_type=MESH)
    for dx in range(1, NX):
        pl.semaphore_signal(barrier, inc=1, device_id=xpeer(dx), device_id_type=MESH)
    pl.semaphore_signal(barrier, inc=1, device_id=partner, device_id_type=MESH)

    first = tile_of(x)
    start = pl.multiple_of(z * PLANE, LANES)
    hstart = pl.multiple_of(z * PLANE + first * LANES, LANES)
    offset = lax.rem(96 * x, LANES)
    wide = jnp.logical_or(x == 1, x == 2)

    def own_block(a):
        return pltpu.make_async_copy(
            weights[a].at[:, pl.ds(start, PLANE)], zbuf.at[0, a], local_sem.at[a]
        )

    def early_block(k):
        dz, a = EARLY[k]
        column = pl.multiple_of(lax.rem(z + dz, NZ) * PLANE, LANES)
        return pltpu.make_async_copy(
            weights[a].at[:, pl.ds(column, PLANE)], early.at[k], local_sem.at[9 + k]
        )

    highs = (high_gate, high_up)

    def own_high(a):
        return pltpu.make_async_copy(
            highs[a].at[:, pl.ds(hstart, NEAR)],
            hbuf.at[a, :, pl.ds(0, NEAR)],
            local_sem.at[2 + a],
        )

    def own_high_rest(a):
        rest = pl.multiple_of(hstart + NEAR, LANES)
        return pltpu.make_async_copy(
            highs[a].at[:, pl.ds(rest, LANES)],
            hbuf.at[a, :, pl.ds(NEAR, LANES)],
            local_sem.at[4 + a],
        )

    lows = (low_gate, low_up)

    def own_low(a):
        return pltpu.make_async_copy(lows[a], lowown, local_sem.at[6])

    norms = (norm_train, norm_step)

    def own_norm(k):
        return pltpu.make_async_copy(norms[k], normbuf.at[0, 0, 0, k], local_sem.at[7 + k])

    for a in range(2):

        @pl.when(core == a)
        def _():
            own_low(a).start()

    for a in range(2):
        own_block(a).start()
    for k in range(len(EARLY)):
        early_block(k).start()
    for a in range(2):
        own_high(a).start()

        @pl.when(wide)
        def _():
            own_high_rest(a).start()

        own_norm(a).start()

    lowbuf[0, 0, 0] = jnp.zeros((RANK, LANES), jnp.bfloat16)
    own_low(0).wait()
    lowbuf[0, 0, 0, :, :ROWS] = lowown[...]

    pl.semaphore_wait(barrier, NZ - 1 + NX - 1 + 1)

    def low_z(dz):
        return remote(lowbuf.at[0, 0, 0], lowbuf.at[0, 0, dz], lzs.at[dz], lzr.at[dz], zpeer(dz))

    def norm_z(k, dz):
        return remote(
            norms[k], normbuf.at[0, 0, dz, k], nzs.at[dz, k], nzr.at[dz, k], zpeer(dz)
        )

    def block_z(i):
        dz, a, row, count = PIECES[i]
        column = pl.multiple_of(lax.rem(z + dz, NZ) * PLANE, LANES)
        return remote(
            weights[a].at[pl.ds(row, count), pl.ds(column, PLANE)],
            zbuf.at[dz, a, pl.ds(row, count)],
            zs.at[i],
            zr.at[i],
            zpeer(dz),
        )

    for dz in ORDER:
        low_z(dz).start()
    for dz in ORDER:
        for k in range(2):
            norm_z(k, dz).start()
    for i in range(len(PIECES)):
        block_z(i).start()

    def slot_row(dz, there):
        plane = lax.rem(z + NZ - dz, NZ)
        return pl.multiple_of(there * ROWS + lax.rem(plane, 2) * HALF, 16)

    def block_x(i, dx):
        dz, a, row, count = ALL[i]
        there = lax.rem(x + dx, NX)
        target = pl.multiple_of(slot_row(dz, x) + row, 16)
        return remote(
            pack.at[dz, a, there, pl.ds(row, count)],
            xbuf.at[a, dz, pl.ds(target, count)],
            xs.at[i, dx],
            xr.at[i, dx],
            xpeer(dx),
        )

    def columns_for(source, rows, there):
        begin, shift = divmod(there * COLS, LANES)
        width = min(WIDE, PLANE - begin * LANES)
        if not shift:
            return source[rows, pl.ds(0, NEAR)]
        taken = source[rows, pl.ds(begin * LANES, width)].astype(jnp.float32)
        return pltpu.roll(taken, width - shift, 1)[:, :NEAR].astype(jnp.bfloat16)

    def early_x(k, dx):
        there = lax.rem(x + dx, NX)
        return remote(
            earlypack.at[k, there],
            earlyrow.at[k, pl.ds(pl.multiple_of(x * ROWS, 16), ROWS)],
            exs.at[k, dx],
            exr.at[k, dx],
            xpeer(dx),
        )

    def early_z(k):
        dz, a = EARLY[k]
        row = pl.multiple_of(lax.rem(z, 2) * HALF, HALF)
        return remote(
            earlyrow.at[k], xbuf.at[a, dz, pl.ds(row, NX * ROWS)], ezs.at[k], ezr.at[k], zpeer(dz)
        )

    def early_start(k):
        early_block(k).wait()
        for there in range(NX):
            moved = columns_for(early.at[k], pl.ds(0, ROWS), there)
            earlypack[k, there] = moved

            @pl.when(x == there)
            def _():
                earlyrow[k, there * ROWS : (there + 1) * ROWS] = moved

        for dx in (1, 3, 2):
            early_x(k, dx).start()

    def early_on(k):
        for dx in (1, 3, 2):
            early_x(k, dx).wait_recv()
        early_z(k).start()

    def forward(i):
        dz, a, row, count = ALL[i]
        target = pl.multiple_of(slot_row(dz, x) + row, 16)
        rows = pl.ds(row, count)
        for there in range(NX):
            moved = columns_for(zbuf.at[dz, a], rows, there)
            pack[dz, a, there, rows] = moved

            @pl.when(x == there)
            def _():
                xbuf[a, dz, pl.ds(target, count)] = moved

        for dx in (1, 3, 2):
            block_x(i, dx).start()

    def low_x(dx):
        return remote(lowbuf.at[0, 0], lowbuf.at[0, dx], lxs.at[dx], lxr.at[dx], xpeer(dx))

    def norm_x(dx):
        return remote(normbuf.at[0, 0], normbuf.at[0, dx], nxs.at[dx], nxr.at[dx], xpeer(dx))

    def low_core():
        return remote(lowbuf.at[0], lowbuf.at[1], ds.at[0], dr.at[0], partner)

    def norm_core():
        return remote(normbuf.at[0], normbuf.at[1], ds.at[1], dr.at[1], partner)

    for a in range(2):
        for dz in range(NZ):
            odd = lax.rem(z + NZ - dz, NZ)
            spare = pl.ds(pl.multiple_of((1 - lax.rem(odd, 2)) * NX * ROWS, HALF), HALF)
            xbuf[a, dz, spare] = jnp.zeros((HALF, NEAR), jnp.bfloat16)
            lowrows[a, dz, spare] = jnp.zeros((HALF, RANK), jnp.bfloat16)

    for k in range(len(EARLY)):
        early_start(k)
    for a in range(2):
        own_block(a).wait()
        forward(a)
    for a in range(2):
        own_norm(a).wait()
        own_high(a).wait()

        @pl.when(wide)
        def _():
            own_high_rest(a).wait()

        @pl.when(jnp.logical_not(wide))
        def _():
            hbuf[a, :, NEAR:] = jnp.zeros((RANK, LANES), jnp.bfloat16)

    low = pl.multiple_of(offset, 32)
    row_of = lax.broadcasted_iota(jnp.int32, (COLS, NEAR), 0)
    lane_of = lax.broadcasted_iota(jnp.int32, (COLS, NEAR), 1)
    pick[...] = jnp.where(lane_of == row_of, 1.0, 0.0).astype(jnp.bfloat16)
    for a in range(2):
        hturn[...] = hbuf[a].astype(jnp.float32).T
        hcols[a] = hturn[pl.ds(low, COLS), :].astype(jnp.bfloat16)
        peak[a] = jnp.zeros((COLS, LANES), jnp.float32)

    def turn_low():
        for a in range(2):
            held = jnp.where(core == a, 0, 1)

            @pl.loop(0, NX)
            def _(dx):
                there = lax.rem(x + NX - dx, NX)

                @pl.loop(0, NZ)
                def _(dz):
                    block = lowbuf[held, dx, dz].astype(jnp.float32).T[:ROWS]
                    lowrows[a, dz, pl.ds(slot_row(dz, there), ROWS)] = block.astype(jnp.bfloat16)

    def merge(a, dz):
        if (dz, a) in EARLY:
            early_z(EARLY.index((dz, a))).wait_recv()
        for i, piece in enumerate(ALL):
            if piece[:2] == (dz, a):
                for dx in (1, 3, 2):
                    block_x(i, dx).wait_recv()
        plane = lax.rem(z + NZ - dz, NZ) * SLOT
        turned = (((1,), (1,)), ((), ()))
        for half in range(0, SLOT, NEAR):
            base = lax.dot_general(
                pick[...],
                xbuf[a, dz, half : half + NEAR, :],
                turned,
                preferred_element_type=jnp.float32,
            )
            product = lax.dot_general(
                hcols[a],
                lowrows[a, dz, half : half + NEAR, :],
                turned,
                preferred_element_type=jnp.float32,
            )
            value = base + mix_rate * product
            fresh[a][:, pl.ds(pl.multiple_of(plane + half, NEAR), NEAR)] = value
            size = jnp.abs(value)
            peak[a] = jnp.maximum(peak[a], jnp.maximum(size[:, :LANES], size[:, LANES:]))

    def gather_norm():
        @pl.loop(0, NX)
        def _(dx):
            @pl.loop(0, NZ)
            def _(dz):
                who = lax.rem(z + NZ - dz, NZ) * NX + lax.rem(x + NX - dx, NX)
                for c in range(2):
                    side = core if c == 0 else 1 - core
                    total = normbuf[c, dx, dz, 0] + normbuf[c, dx, dz, 1]
                    norm_abs[pl.ds(who * 2 + side, 1), pl.ds(0, NORM)] = total

        rows = [jnp.zeros((4, LANES), jnp.float32) for _ in range(7)]
        lane = lax.broadcasted_iota(jnp.int32, (4, LANES), 1)
        for j in range(16):
            begin = NORM * j
            row, shift = begin // LANES, begin % LANES
            taken = norm_abs[pl.ds(j, 4, stride=16), :]
            moved = pltpu.roll(taken, shift, 1) if shift else taken
            end = shift + NORM
            inside = jnp.logical_and(lane >= shift, lane < end)
            rows[row] = jnp.where(inside, moved, rows[row])
            if end > LANES:
                rows[row + 1] = jnp.where(lane < end - LANES, moved, rows[row + 1])
        for q in range(7):
            norm_acc[pl.ds(q, 4, stride=7), :] = rows[q]
        norm_out[...] = norm_acc[...].astype(jnp.bfloat16)

    blocks = [piece[:2] for piece in ALL] + list(EARLY)
    done = 0
    for i, (dz, a, row, count) in enumerate(PIECES):
        block_z(i).wait_recv()
        forward(len(OWN) + i)
        if i < len(EARLY):
            early_on(i)
        if i == 2:
            for far in ORDER:
                low_z(far).wait_recv()
            for dx in (1, 3, 2):
                low_x(dx).start()
        if i == 4:
            for dx in (1, 3, 2):
                low_x(dx).wait_recv()
            low_core().start()
        if i == 6:
            low_core().wait_recv()
            turn_low()
        if i == 4:
            for far in ORDER:
                for k in range(2):
                    norm_z(k, far).wait_recv()
            for dx in (1, 3, 2):
                norm_x(dx).start()
        if i == 6:
            for dx in (1, 3, 2):
                norm_x(dx).wait_recv()
            norm_core().start()
        if i == 8:
            norm_core().wait_recv()
            gather_norm()
        if i >= 6:
            for _ in range(3):
                if blocks[done] != (dz, a):
                    merge(blocks[done][1], blocks[done][0])
                    done += 1
    while done < len(blocks):
        merge(blocks[done][1], blocks[done][0])
        done += 1

    for k in range(len(EARLY)):
        early_z(k).wait_send()
        for dx in (1, 3, 2):
            early_x(k, dx).wait_send()
    for i in range(len(PIECES)):
        block_z(i).wait_send()
    for dz in ORDER:
        low_z(dz).wait_send()
        for k in range(2):
            norm_z(k, dz).wait_send()
    for dx in (1, 3, 2):
        low_x(dx).wait_send()
        norm_x(dx).wait_send()
        for i in range(len(ALL)):
            block_x(i, dx).wait_send()
    low_core().wait_send()
    norm_core().wait_send()


CHUNK = 32


def finish_kernel(
    fresh_gate,
    fresh_up,
    peak,
    norm,
    serve_gate,
    serve_up,
    column_gate,
    column_up,
    serve_norm,
    held,
    sem,
):
    targets = (serve_gate, serve_up)
    columns = (column_gate, column_up)
    for a, source in enumerate((fresh_gate, fresh_up)):

        @pl.loop(0, COLS // CHUNK)
        def _(i):
            rows = pl.ds(pl.multiple_of(i * CHUNK, CHUNK), CHUNK)
            scale = 1.0 / jnp.max(peak[a, rows, :], axis=1, keepdims=True)
            for pair in range(NZ // 2):
                even = source[rows, pl.ds(2 * pair * SLOT, SLOT)]
                odd = source[rows, pl.ds((2 * pair + 1) * SLOT, SLOT)]
                begin = 2 * pair * NX * ROWS
                parts = (even[:, :WIDE], even[:, WIDE:] + odd[:, :LANES], odd[:, LANES:])
                for part in parts:
                    width = part.shape[1]
                    held[a, rows, pl.ds(begin, width)] = (part * scale).astype(jnp.bfloat16)
                    begin += width
            pltpu.make_async_copy(held.at[a, rows], targets[a].at[rows], sem.at[a, i]).start()

    for a in range(2):
        columns[a][...] = jnp.max(peak[a].T, axis=0, keepdims=True)
    serve_norm[...] = norm[...]
    for a in range(2):

        @pl.loop(0, COLS // CHUNK)
        def _(i):
            rows = pl.ds(pl.multiple_of(i * CHUNK, CHUNK), CHUNK)
            pltpu.make_async_copy(held.at[a, rows], targets[a].at[rows], sem.at[a, i]).wait()


def local(w_gate, low_gate, high_gate, w_up, low_up, high_up, norm_train, norm_step):
    anywhere = pl.BlockSpec(memory_space=pl.ANY)
    vmem = pl.BlockSpec(memory_space=pltpu.VMEM)
    dma = pltpu.SemaphoreType.DMA
    def outside(v):
        return pltpu.with_memory_space_constraint(v, pltpu.HBM)

    fresh_gate, fresh_up, peak, norm = pl.pallas_call(
        exchange_kernel,
        name="exchange",
        out_shape=(
            pltpu.VMEM((COLS, NZ * SLOT), jnp.float32),
            pltpu.VMEM((COLS, NZ * SLOT), jnp.float32),
            pltpu.VMEM((2, COLS, LANES), jnp.float32),
            pltpu.VMEM((28, LANES), jnp.bfloat16),
        ),
        in_specs=[anywhere] * 8,
        out_specs=(vmem,) * 4,
        scratch_shapes=[
            pltpu.VMEM((NZ, 2, ROWS, PLANE), jnp.bfloat16),
            pltpu.VMEM((NZ, 2, NX, ROWS, NEAR), jnp.bfloat16),
            pltpu.VMEM((2, NZ, SLOT, NEAR), jnp.bfloat16),
            pltpu.VMEM((len(EARLY), ROWS, PLANE), jnp.bfloat16),
            pltpu.VMEM((len(EARLY), NX, ROWS, NEAR), jnp.bfloat16),
            pltpu.VMEM((len(EARLY), NX * ROWS, NEAR), jnp.bfloat16),
            pltpu.VMEM((RANK, ROWS), jnp.bfloat16),
            pltpu.VMEM((2, NX, NZ, RANK, LANES), jnp.bfloat16),
            pltpu.VMEM((2, NZ, SLOT, RANK), jnp.bfloat16),
            pltpu.VMEM((2, NX, NZ, 2, 1, NORM), jnp.float32),
            pltpu.VMEM((2, RANK, WIDE), jnp.bfloat16),
            pltpu.VMEM((WIDE, RANK), jnp.float32),
            pltpu.VMEM((COLS, NEAR), jnp.bfloat16),
            pltpu.VMEM((2, COLS, RANK), jnp.bfloat16),
            pltpu.VMEM((64, LANES), jnp.float32),
            pltpu.VMEM((28, LANES), jnp.float32),
            dma((9 + len(EARLY),)),
            dma((len(PIECES),)),
            dma((len(PIECES),)),
            dma((len(ALL), NX)),
            dma((len(ALL), NX)),
            dma((NZ,)),
            dma((NZ,)),
            dma((NX,)),
            dma((NX,)),
            dma((NZ, 2)),
            dma((NZ, 2)),
            dma((NX,)),
            dma((NX,)),
            dma((2,)),
            dma((2,)),
            dma((len(EARLY), NX)),
            dma((len(EARLY), NX)),
            dma((len(EARLY),)),
            dma((len(EARLY),)),
        ],
        compiler_params=pltpu.CompilerParams(
            collective_id=0, has_side_effects=True, vmem_limit_bytes=32 * 1024 * 1024
        ),
    )(
        outside(w_gate),
        outside(low_gate.T),
        outside(high_gate),
        outside(w_up),
        outside(low_up.T),
        outside(high_up),
        outside(norm_train.reshape(1, NORM)),
        outside(norm_step.reshape(1, NORM)),
    )
    inside = [
        pltpu.with_memory_space_constraint(v, pltpu.VMEM)
        for v in (fresh_gate, fresh_up, peak, norm)
    ]
    serve_gate, serve_up, column_gate, column_up, serve_norm = pl.pallas_call(
        finish_kernel,
        name="finish",
        out_shape=(
            jax.ShapeDtypeStruct((COLS, TOTAL), jnp.bfloat16),
            jax.ShapeDtypeStruct((COLS, TOTAL), jnp.bfloat16),
            jax.ShapeDtypeStruct((1, COLS), jnp.float32),
            jax.ShapeDtypeStruct((1, COLS), jnp.float32),
            jax.ShapeDtypeStruct((28, LANES), jnp.bfloat16),
        ),
        in_specs=[vmem] * 4,
        out_specs=(anywhere, anywhere, vmem, vmem, vmem),
        scratch_shapes=[
            pltpu.VMEM((2, COLS, TOTAL), jnp.bfloat16),
            dma((2, COLS // CHUNK)),
        ],
        compiler_params=pltpu.CompilerParams(vmem_limit_bytes=16 * 1024 * 1024),
    )(*inside)
    return (
        serve_gate.T,
        serve_up.T,
        column_gate.reshape(COLS),
        column_up.reshape(COLS),
        serve_norm.reshape(28 * LANES),
    )


def solution(mesh):
    rows = ("unit", "shard")
    return jax.shard_map(
        local,
        mesh=mesh,
        in_specs=(
            P(rows, "width"),
            P(rows, None),
            P("unit", "width"),
            P(rows, "width"),
            P(rows, None),
            P("unit", "width"),
            P(("unit", "shard", "width")),
            P(("unit", "shard", "width")),
        ),
        out_specs=(
            P("unit", ("width", "shard")),
            P("unit", ("width", "shard")),
            P(("unit", "width", "shard")),
            P(("unit", "width", "shard")),
            P("unit"),
        ),
        check_vma=False,
    )
```
